32 devices in a mesh: gx: 2 (over y), gy: 4 (over x, core), gz: 4 (over z).
Axes of the slice: x: 2, y: 2, z: 4, core: 2. Of those that a mesh axis runs over, the one named last changes fastest.
Arguments:
- probe_bits: int32 [8, 32, 512], P('gx', 'gz', 'gy'), may hold values from -2147483648 to 2147483646
- disorder_levels: int32 [8, 32, 512], P('gx', 'gz', 'gy'), may hold values from -2147483648 to 2147483647, as said below
Outputs:
- moments: float32 [3, 8], replicated
- previous: float32 [8, 8, 128, 512], P(None, 'gx', 'gz', 'gy')
- current: float32 [8, 8, 128, 512], P(None, 'gx', 'gz', 'gy')
The draws below stay inside these ranges and needn't reach their ends.
Inputs may be any that keep to these rules, and one draw needn't show every extreme that they name: `disorder_levels`: every byte of a word is a level 0 to 255.
All inputs are finite; a program needn't handle non-finite values.
Results may differ from the reference program's by a relative error of at most 0.00002.
Values sent between devices are 32-bit elements; how exact they have to be, the bound alone decides.
A program may use at most 64 MiB of HBM per device.

```python
import jax
import jax.numpy as jnp
from jax import lax

PROBES = 8
LEVELS = 256
NX = 8
NY = 512
NZ = 128
NSITES = 524288


def draw_disorder_levels(key, part):
    shape = (NX, NZ, NY)
    group = jax.random.randint(jax.random.fold_in(key, 11), (), 0, 2)
    base = 32 + jax.random.randint(jax.random.fold_in(key, 12), (), 0, 64) + 128 * group
    slope = 32 * (2 * jax.random.randint(jax.random.fold_in(key, 13), (), 0, 2) - 1)
    offsets = jax.random.randint(jax.random.fold_in(key, 14), (4, 4, 4), -16, 17)
    widths = jax.random.randint(jax.random.fold_in(key, 15), (4, 4, 4), 16, 80)
    patch_x = lax.broadcasted_iota(jnp.int32, shape, 0) * 4 // NX
    patch_z = lax.broadcasted_iota(jnp.int32, shape, 1) * 4 // NZ
    patch_y = lax.broadcasted_iota(jnp.int32, shape, 2) * 4 // NY
    local_offset = offsets[patch_x, patch_z, patch_y]
    local_width = widths[patch_x, patch_z, patch_y]
    centre = base + slope * (patch_x - 1) + local_offset
    raw = jax.random.randint(jax.random.fold_in(key, 16), shape, 0, 161)
    jitter = raw % (2 * local_width + 1) - local_width
    patchy = jnp.clip(centre + jitter, 0, LEVELS - 1)
    background = jax.random.randint(jax.random.fold_in(key, 17), shape, 0, LEVELS)
    picker = jax.random.randint(jax.random.fold_in(key, 18), shape, 0, 8)
    levels = jnp.where(picker == 0, background, patchy).astype(jnp.int32)
    grouped = levels.reshape(NX, NZ // 4, 4, NY)
    top_byte = grouped[:, :, 3, :]
    top_signed = jnp.where(top_byte >= 128, top_byte - 256, top_byte)
    packed = grouped[:, :, 0, :] + grouped[:, :, 1, :] * 256 + grouped[:, :, 2, :] * 65536 + top_signed * 16777216
    return packed.astype(jnp.int32)


def plant(entries, rng, low, top_value):
    shape = entries.shape
    place = [jax.random.randint(jax.random.fold_in(rng, axis), (), 0, shape[axis]) for axis in range(len(shape))]
    entries = entries.at[tuple(place)].set(low)
    longest = shape.index(max(shape))
    place[longest] = (place[longest] + 1) % shape[longest]
    return entries.at[tuple(place)].set(top_value)


def shard_levels(stream_key, extent, cuts, smallest, top_value):
    factor_of, own = 1.0, jax.random.fold_in(stream_key, 6)
    for axis_at, parts in cuts:
        heights = jnp.exp(jax.random.uniform(jax.random.fold_in(own, axis_at), (parts,), jnp.float32, smallest / len(cuts), top_value / len(cuts)))
        factor_of = factor_of * jnp.repeat(heights, extent[axis_at] // parts).reshape([-1 if axis == axis_at else 1 for axis in range(len(extent))])
    return factor_of


def setup_inputs(seed: int = 0) -> dict:
    seeds = jax.random.split(jax.random.key(seed), 3)
    probe_bits = plant(jax.random.randint(seeds[0], (NX, NZ // 4, NY), -2147483648, 2147483647), jax.random.fold_in(seeds[0], 1), -2147483648, 2147483646).astype(jnp.int32)
    disorder_levels = draw_disorder_levels(jax.random.fold_in(seeds[2], 71), 0)
    return dict(probe_bits=probe_bits, disorder_levels=disorder_levels)


disorder_width = 4.0
spectral_scale = 8.4


def unpack_signs(packed):
    shifts = 4 * jnp.arange(PROBES, dtype=jnp.int32)[:, None] + jnp.arange(4, dtype=jnp.int32)[None, :]
    bit_values = jnp.right_shift(packed[None, :, :, None, :], shifts[:, None, None, :, None]) & 1
    layout = bit_values.shape
    flat = bit_values.reshape(layout[0], layout[1], layout[2] * layout[3], layout[4])
    return 2.0 * flat.astype(jnp.float32) - 1.0


def unpack_energy(packed):
    shifts = 8 * jnp.arange(4, dtype=jnp.int32)
    levels = jnp.right_shift(packed[:, :, None, :], shifts[None, None, :, None]) & 255
    layout = levels.shape
    flat = levels.reshape(layout[0], layout[1] * layout[2], layout[3])
    return disorder_width * ((flat.astype(jnp.float32) + 0.5) / LEVELS - 0.5)


def apply_ham(field, energy):
    beside = jnp.roll(field, -1, 1) + jnp.roll(field, 1, 1)
    beside = beside + jnp.roll(field, -1, 3) + jnp.roll(field, 1, 3)
    beside = beside + jnp.roll(field, -1, 2) + jnp.roll(field, 1, 2)
    return (energy[None] * field - beside) / spectral_scale


def reference(probe_bits, disorder_levels):
    signs = unpack_signs(probe_bits)
    energy = unpack_energy(disorder_levels)
    first = apply_ham(signs, energy)
    second = 2.0 * apply_ham(first, energy) - signs
    third = 2.0 * apply_ham(second, energy) - first
    moments = jnp.stack([jnp.sum(signs * vec, axis=(1, 2, 3)) for vec in (first, second, third)]) / NSITES
    return moments, second, third
```

```python
import functools

import jax
import jax.numpy as jnp
from jax import lax
from jax.experimental import pallas as pl
from jax.experimental.pallas import tpu as pltpu
from jax.sharding import PartitionSpec as P

PROBES = 8
LEVELS = 256
LANES = 128
SITES = 4
STRIP = 12

disorder_width = 4.0
spectral_scale = 8.4
MESH = pl.DeviceIdType.MESH


def kernel(names, sizes, p_ref, d_ref, prow_ref, drow_ref, mom_ref, prev_ref, cur_ref,
           words, packs, strips, v0, v1, v2, en, s0, s1, s2, se, moms,
           send_sem, recv_sem, msend_sem, mrecv_sem):
    X, W, _ = p_ref.shape
    Z = SITES * W
    nbx = packs.shape[0]
    M = nbx * X
    gx, gy, gz = sizes["gx"], sizes["gy"], sizes["gz"]
    ix, iy, iz = (lax.axis_index(a) for a in ("gx", "gy", "gz"))
    total = gx * gy * gz
    me = (ix * gy + iy) * gz + iz

    def device(x, y, z):
        at = {"gx": x, "gy": y, "gz": z}
        return tuple(at[a] for a in names)

    def nth(k):
        t = lax.rem(me + k, total)
        return device(t // (gy * gz), lax.rem(t // gz, gy), lax.rem(t, gz)), t

    barrier = pltpu.get_barrier_semaphore()

    def greet(k, _):
        pl.semaphore_signal(barrier, inc=1, device_id=nth(k)[0], device_id_type=MESH)
        return 0

    lax.fori_loop(1, total, greet, 0)

    lane = lax.broadcasted_iota(jnp.int32, (2 * X, LANES), 1)
    slot_word = (lane * 10923) >> 17
    column = lane - STRIP * slot_word

    pack = jnp.zeros((2 * X, LANES), jnp.int32)
    for w in range(W):
        rows = jnp.concatenate([p_ref[:, w, :], d_ref[:, w, :]], axis=0)
        base = STRIP * (w + 1)
        first = pltpu.roll(rows, (base - (LANES - 3)) % LANES, 1)
        second = pltpu.roll(rows, (base + 5 - (LANES - 2)) % LANES, 1)
        pack = jnp.where(slot_word == w + 1, jnp.where(column < 5, first, second), pack)
    packs[0, 1, 1] = pack
    for f, ref in enumerate((prow_ref, drow_ref)):
        words[f, 0:X, 1:W + 1] = ref[...]

    pl.semaphore_wait(barrier, total - 1)

    xs = (0, 1) if nbx == 2 else (0, 1, -1)
    slot_of = {0: 0, 1: nbx - 1, -1: 1}
    copies = []
    for ox in xs:
        for oz in (0, 1, -1):
            for oy in (0, 1, -1):
                if ox == 0 and oz == 0 and oy == 0:
                    continue
                to = device(lax.rem(ix + ox + gx, gx), lax.rem(iy + oy + gy, gy), lax.rem(iz + oz + gz, gz))
                s = slot_of[ox]
                moves = []
                if oy == 0:
                    src_w, dst_w = {0: (pl.ds(0, W), pl.ds(1, W)), 1: (pl.ds(W - 1, 1), pl.ds(0, 1)),
                                    -1: (pl.ds(0, 1), pl.ds(W + 1, 1))}[oz]
                    for f, ref in enumerate((prow_ref, drow_ref)):
                        moves.append((ref.at[:, src_w], words.at[f, pl.ds(s * X, X), dst_w]))
                moves.append((packs.at[0, 1, 1], packs.at[s, 1 - oz, 1 - oy]))
                for src, dst in moves:
                    n = len(copies)
                    copies.append(pltpu.make_async_remote_copy(
                        src_ref=src, dst_ref=dst, send_sem=send_sem.at[n], recv_sem=recv_sem.at[n],
                        device_id=to, device_id_type=MESH))
    for copy in copies:
        copy.start()
    for copy in copies:
        copy.wait()

    scale = 1.0 / spectral_scale
    e_mul = disorder_width / LEVELS / spectral_scale
    e_add = disorder_width * (0.5 / LEVELS - 0.5) / spectral_scale
    probe = lax.broadcasted_iota(jnp.int32, (PROBES, LANES), 0)
    lane8 = lax.broadcasted_iota(jnp.int32, (PROBES, LANES), 1)
    col8 = lane8 - STRIP * ((lane8 * 10923) >> 17)
    lifts = [31 - (SITES * probe + j) for j in range(SITES)]

    def sign_of(row, j):
        return jnp.where((jnp.broadcast_to(row, (PROBES, LANES)) << lifts[j]) < 0, 1.0, -1.0).astype(jnp.float32)

    def energy_of(row, j):
        level = (jnp.broadcast_to(row, (PROBES, LANES)) >> (8 * j)) & 255
        return level.astype(jnp.float32) * e_mul + e_add

    for s in range(nbx):
        def joined(oz):
            return jnp.where(column < 3, packs[s, oz, 0], jnp.where(column < 7, packs[s, oz, 1], packs[s, oz, 2]))
        strip = jnp.where(slot_word == 0, pltpu.roll(joined(0), (-STRIP * W) % LANES, 1), joined(1))
        strips[s] = jnp.where(slot_word == W + 1, pltpu.roll(joined(2), (STRIP * W) % LANES, 1), strip)
        for x in range(X):
            for j in range(SITES):
                s0[s * X + x, j] = sign_of(strips[s, x:x + 1], j)
                se[s * X + x, j] = energy_of(strips[s, X + x:X + x + 1], j)

    def plane(e):
        return lax.rem(e + M, M)

    def unpack(i, _):
        q = plane(i - 3)
        for z in range(-3, Z + 3):
            w, j = divmod(z + SITES, SITES)
            v0[q, z + 3] = sign_of(words[0, q, w], j)
            en[q, z + 3] = energy_of(words[1, q, w], j)
        return 0

    lax.fori_loop(0, min(M, X + 6), unpack, 0)

    def strip_sum(src, q, up, down):
        mine = [src[q, j] for j in range(SITES)]
        sums = []
        for j in range(SITES):
            z_up = mine[j + 1] if j + 1 < SITES else pltpu.roll(mine[0], LANES - STRIP, 1)
            z_down = mine[j - 1] if j > 0 else pltpu.roll(mine[SITES - 1], STRIP, 1)
            sums.append(src[up, j] + src[down, j] + pltpu.roll(mine[j], LANES - 1, 1)
                        + pltpu.roll(mine[j], 1, 1) + z_up + z_down)
        return mine, sums

    def edges_of(mine):
        return [jnp.where(col8 == 1, pltpu.roll(m, LANES - 6, 1), m) for m in mine]

    def site_sum(src, q, up, down, z, edges):
        w, j = divmod(z + SITES, SITES)
        fix = pltpu.roll(edges[j], (-(STRIP * w + 2)) % LANES, 1)
        mid = src[q, z + 3]
        right = jnp.where(lane8 == LANES - 1, fix, pltpu.roll(mid, LANES - 1, 1))
        left = jnp.where(lane8 == 0, fix, pltpu.roll(mid, 1, 1))
        return mid, src[up, z + 3] + src[down, z + 3] + right + left + src[q, z + 4] + src[q, z + 2]

    zero = jnp.zeros((PROBES, LANES), jnp.float32)

    def first_level(i, accs):
        e = i - 2
        q, up, down = plane(e), plane(e + 1), plane(e + M - 1)
        mine, sums = strip_sum(s0, q, up, down)
        for j in range(SITES):
            s1[q, j] = se[q, j] * mine[j] - scale * sums[j]
        edges = edges_of(mine)
        one, two = zero, zero
        for z in range(-2, Z + 2):
            mid, total_six = site_sum(v0, q, up, down, z, edges)
            new = en[q, z + 3] * mid - scale * total_six
            v1[q, z + 3] = new
            if 0 <= z < Z:
                one, two = one + mid * new, two + new * new
        own = jnp.where((e >= 0) & (e < X), 1.0, 0.0).astype(jnp.float32)
        return accs[0] + own * one, accs[1] + own * two

    m1, m2 = lax.fori_loop(0, min(M, X + 4), first_level, (zero, zero))

    def second_level(i, acc):
        e = i - 1
        q, up, down = plane(e), plane(e + 1), plane(e + M - 1)
        mine, sums = strip_sum(s1, q, up, down)
        for j in range(SITES):
            s2[q, j] = 2.0 * (se[q, j] * mine[j] - scale * sums[j]) - s0[q, j]
        edges = edges_of(mine)
        three = zero
        for z in range(-1, Z + 1):
            mid, total_six = site_sum(v1, q, up, down, z, edges)
            new = 2.0 * (en[q, z + 3] * mid - scale * total_six) - v0[q, z + 3]
            v2[q, z + 3] = new
            if 0 <= z < Z:
                three = three + mid * new
        own = jnp.where((e >= 0) & (e < X), 1.0, 0.0).astype(jnp.float32)
        return acc + own * three

    m3 = lax.fori_loop(0, X + 2, second_level, zero)

    row = zero
    for n, acc in enumerate((m1, m2, m3)):
        summed = jnp.broadcast_to(jnp.sum(acc, axis=1, keepdims=True), (PROBES, LANES))
        row = row + jnp.where(lane8 == PROBES * n + probe, summed, 0.0)
    moms[me] = jnp.sum(row, axis=0, keepdims=True)

    def moment_copy(k):
        to, t = nth(k)
        out = pltpu.make_async_remote_copy(
            src_ref=moms.at[me], dst_ref=moms.at[me], send_sem=msend_sem.at[t], recv_sem=mrecv_sem.at[me],
            device_id=to, device_id_type=MESH)
        back = pltpu.make_async_remote_copy(
            src_ref=moms.at[me], dst_ref=moms.at[t], send_sem=msend_sem.at[t], recv_sem=mrecv_sem.at[t],
            device_id=to, device_id_type=MESH)
        return out, back

    def send(k, _):
        moment_copy(k)[0].start()
        return 0

    lax.fori_loop(1, total, send, 0)

    def third_level(x, _):
        q, up, down = plane(x), plane(x + 1), plane(x + M - 1)
        edges = edges_of([s2[q, j] for j in range(SITES)])
        for z in range(Z):
            mid, total_six = site_sum(v2, q, up, down, z, edges)
            new = 2.0 * (en[q, z + 3] * mid - scale * total_six) - v1[q, z + 3]
            at = pl.ds(x * Z + z, PROBES, stride=X * Z)
            prev_ref[at, :] = mid
            cur_ref[at, :] = new
        return 0

    lax.fori_loop(0, X, third_level, 0)

    def land(k, _):
        out, back = moment_copy(k)
        out.wait_send()
        back.wait_recv()
        return 0

    lax.fori_loop(1, total, land, 0)
    sites = total * X * Z * LANES
    sums = jnp.sum(moms[...], axis=0) * (1.0 / sites)
    first = sums
    second = 2.0 * pltpu.roll(sums, LANES - PROBES, 1) - 1.0
    third = 2.0 * pltpu.roll(sums, LANES - 2 * PROBES, 1) - sums
    mom_ref[...] = jnp.concatenate([first, second, third], axis=0)[:, :PROBES]


def per_device(names, sizes, probe_bits, disorder_levels):
    X, W, Y = probe_bits.shape
    if Y != LANES or STRIP * (W + 2) > LANES or X < 3:
        raise ValueError("block size")
    Z = SITES * W
    nbx = 2 if sizes["gx"] == 2 else 3
    M = nbx * X
    n_copies = (9 * nbx - 1) + 2 * (3 * nbx - 1)
    total = sizes["gx"] * sizes["gy"] * sizes["gz"]
    rows = (X, W, 1, Y)
    vmem = pl.BlockSpec(memory_space=pltpu.VMEM)
    f32, i32 = jnp.float32, jnp.int32
    tile = (PROBES, LANES)
    moments, previous, current = pl.pallas_call(
        functools.partial(kernel, names, sizes),
        out_shape=(
            jax.ShapeDtypeStruct((3, PROBES), f32),
            jax.ShapeDtypeStruct((PROBES * X * Z, Y), f32),
            jax.ShapeDtypeStruct((PROBES * X * Z, Y), f32),
        ),
        in_specs=[vmem] * 4,
        out_specs=(vmem,) * 3,
        scratch_shapes=[
            pltpu.VMEM((2, M, W + 2, 1, LANES), i32),
            pltpu.VMEM((nbx, 3, 3, 2 * X, LANES), i32),
            pltpu.VMEM((nbx, 2 * X, LANES), i32),
            pltpu.VMEM((M, Z + 6) + tile, f32),
            pltpu.VMEM((M, Z + 6) + tile, f32),
            pltpu.VMEM((M, Z + 6) + tile, f32),
            pltpu.VMEM((M, Z + 6) + tile, f32),
            pltpu.VMEM((M, SITES) + tile, f32),
            pltpu.VMEM((M, SITES) + tile, f32),
            pltpu.VMEM((M, SITES) + tile, f32),
            pltpu.VMEM((M, SITES) + tile, f32),
            pltpu.VMEM((total, 1, LANES), f32),
            pltpu.SemaphoreType.DMA((n_copies,)),
            pltpu.SemaphoreType.DMA((n_copies,)),
            pltpu.SemaphoreType.DMA((total,)),
            pltpu.SemaphoreType.DMA((total,)),
        ],
        compiler_params=pltpu.CompilerParams(collective_id=0, has_side_effects=True,
                                             vmem_limit_bytes=40 * 1024 * 1024),
    )(probe_bits, disorder_levels, probe_bits.reshape(rows), disorder_levels.reshape(rows))
    shape = (PROBES, X, Z, Y)
    return moments, previous.reshape(shape), current.reshape(shape)


def solution(mesh):
    placed = (P("gx", "gz", "gy"), P("gx", "gz", "gy"))
    sizes = {a: mesh.shape[a] for a in mesh.axis_names}
    return jax.shard_map(
        functools.partial(per_device, tuple(mesh.axis_names), sizes),
        mesh=mesh,
        in_specs=placed,
        out_specs=(P(), P(None, "gx", "gz", "gy"), P(None, "gx", "gz", "gy")),
        check_vma=False,
    )
```

```python
import functools

import jax
import jax.numpy as jnp
from jax import lax
from jax.experimental import pallas as pl
from jax.experimental.pallas import tpu as pltpu
from jax.sharding import PartitionSpec as P

PROBES = 8
LEVELS = 256
LANES = 128
SITES = 4
STRIP = 12

disorder_width = 4.0
spectral_scale = 8.4
MESH = pl.DeviceIdType.MESH


def kernel(names, sizes, p_hbm, d_hbm, prow_hbm, drow_hbm, mom_ref, prev_ref, cur_ref,
           p_ref, d_ref, words, packs, strips, v0, v1, v2, en, s0, s1, s2, se, moms,
           load_sem, send_sem, recv_sem, msend_sem, mrecv_sem):
    X, W, _ = p_ref.shape
    Z = SITES * W
    nbx = packs.shape[0]
    M = nbx * X
    gx, gy, gz = sizes["gx"], sizes["gy"], sizes["gz"]
    ix, iy, iz = (lax.axis_index(a) for a in ("gx", "gy", "gz"))
    total = gx * gy * gz
    me = (ix * gy + iy) * gz + iz

    def device(x, y, z):
        at = {"gx": x, "gy": y, "gz": z}
        return tuple(at[a] for a in names)

    loads = [pltpu.make_async_copy(src, dst, load_sem.at[n]) for n, (src, dst) in enumerate((
        (p_hbm, p_ref), (d_hbm, d_ref),
        (prow_hbm, words.at[0, pl.ds(0, X), pl.ds(1, W)]), (drow_hbm, words.at[1, pl.ds(0, X), pl.ds(1, W)])))]
    for load in loads:
        load.start()

    def around(at, size):
        steps = [at]
        for _ in range(size - 1):
            steps.append(jnp.where(steps[-1] + 1 == size, 0, steps[-1] + 1))
        return steps

    around_x, around_y = around(ix, gx), around(iy, gy)

    def each_other(act):
        for x in range(gx):
            for y in range(gy):
                if x or y:
                    act(device(around_x[x], around_y[y], iz))

        def at_depth(z):
            for x in range(gx):
                for y in range(gy):
                    act(device(around_x[x], around_y[y], z))

        if gz <= 4:
            for z in around(iz, gz)[1:]:
                at_depth(z)
        else:
            def step(k, _):
                at_depth(lax.rem(iz + k, gz))
                return 0
            lax.fori_loop(1, gz, step, 0)

    barrier = pltpu.get_barrier_semaphore()
    each_other(lambda to: pl.semaphore_signal(barrier, inc=1, device_id=to, device_id_type=MESH))

    lane = lax.broadcasted_iota(jnp.int32, (2 * X, LANES), 1)
    slot_word = (lane * 10923) >> 17
    column = lane - STRIP * slot_word

    for load in loads:
        load.wait()
    pack = jnp.zeros((2 * X, LANES), jnp.int32)
    for w in range(W):
        rows = jnp.concatenate([p_ref[:, w, :], d_ref[:, w, :]], axis=0)
        base = STRIP * (w + 1)
        first = pltpu.roll(rows, (base - (LANES - 3)) % LANES, 1)
        second = pltpu.roll(rows, (base + 5 - (LANES - 2)) % LANES, 1)
        pack = jnp.where(slot_word == w + 1, jnp.where(column < 5, first, second), pack)
    packs[0, 1, 1] = pack

    pl.semaphore_wait(barrier, total - 1)

    xs = (0, 1) if nbx == 2 else (0, 1, -1)
    slot_of = {0: 0, 1: nbx - 1, -1: 1}
    copies = []
    for ox in xs:
        for oz in (0, 1, -1):
            for oy in (0, 1, -1):
                if ox == 0 and oz == 0 and oy == 0:
                    continue
                to = device(lax.rem(ix + ox + gx, gx), lax.rem(iy + oy + gy, gy), lax.rem(iz + oz + gz, gz))
                s = slot_of[ox]
                moves = []
                if oy == 0:
                    src_w, dst_w = {0: (pl.ds(1, W), pl.ds(1, W)), 1: (pl.ds(W, 1), pl.ds(0, 1)),
                                    -1: (pl.ds(1, 1), pl.ds(W + 1, 1))}[oz]
                    for f in range(2):
                        moves.append((words.at[f, pl.ds(0, X), src_w], words.at[f, pl.ds(s * X, X), dst_w]))
                moves.append((packs.at[0, 1, 1], packs.at[s, 1 - oz, 1 - oy]))
                for src, dst in moves:
                    n = len(copies)
                    copies.append(pltpu.make_async_remote_copy(
                        src_ref=src, dst_ref=dst, send_sem=send_sem.at[n], recv_sem=recv_sem.at[n],
                        device_id=to, device_id_type=MESH))
    for copy in copies:
        copy.start()
    scale = 1.0 / spectral_scale
    e_mul = disorder_width / LEVELS / spectral_scale
    e_add = disorder_width * (0.5 / LEVELS - 0.5) / spectral_scale
    probe = lax.broadcasted_iota(jnp.int32, (PROBES, LANES), 0)
    lane8 = lax.broadcasted_iota(jnp.int32, (PROBES, LANES), 1)
    col8 = lane8 - STRIP * ((lane8 * 10923) >> 17)
    lifts = [31 - (SITES * probe + j) for j in range(SITES)]

    def sign_of(row, j):
        return jnp.where((jnp.broadcast_to(row, (PROBES, LANES)) << lifts[j]) < 0, 1.0, -1.0).astype(jnp.float32)

    def energy_of(row, j):
        level = (jnp.broadcast_to(row, (PROBES, LANES)) >> (8 * j)) & 255
        return level.astype(jnp.float32) * e_mul + e_add

    def unpack(q, zs):
        for z in zs:
            w, j = divmod(z + SITES, SITES)
            v0[q, z + 3] = sign_of(words[0, q, w], j)
            en[q, z + 3] = energy_of(words[1, q, w], j)

    def unpack_own(x, _):
        unpack(x, range(Z))
        return 0

    lax.fori_loop(0, X, unpack_own, 0)
    for copy in copies:
        copy.wait()

    for s in range(nbx):
        def joined(oz):
            return jnp.where(column < 3, packs[s, oz, 0], jnp.where(column < 7, packs[s, oz, 1], packs[s, oz, 2]))
        strip = jnp.where(slot_word == 0, pltpu.roll(joined(0), (-STRIP * W) % LANES, 1), joined(1))
        strips[s] = jnp.where(slot_word == W + 1, pltpu.roll(joined(2), (STRIP * W) % LANES, 1), strip)
        for x in range(X):
            for j in range(SITES):
                s0[s * X + x, j] = sign_of(strips[s, x:x + 1], j)
                se[s * X + x, j] = energy_of(strips[s, X + x:X + x + 1], j)

    def plane(e):
        return lax.rem(e + M, M)

    def unpack_rim(x, _):
        unpack(x, [*range(-3, 0), *range(Z, Z + 3)])
        return 0

    def unpack_far(i, _):
        unpack(plane(X + i), range(-3, Z + 3))
        return 0

    def unpack_low(i, _):
        unpack(plane(i - 3), range(-3, Z + 3))
        return 0

    lax.fori_loop(0, X, unpack_rim, 0)
    if M <= X + 6:
        lax.fori_loop(0, M - X, unpack_far, 0)
    else:
        lax.fori_loop(0, 3, unpack_far, 0)
        lax.fori_loop(0, 3, unpack_low, 0)

    def strip_sum(src, q, up, down):
        mine = [src[q, j] for j in range(SITES)]
        sums = []
        for j in range(SITES):
            z_up = mine[j + 1] if j + 1 < SITES else pltpu.roll(mine[0], LANES - STRIP, 1)
            z_down = mine[j - 1] if j > 0 else pltpu.roll(mine[SITES - 1], STRIP, 1)
            sums.append(src[up, j] + src[down, j] + pltpu.roll(mine[j], LANES - 1, 1)
                        + pltpu.roll(mine[j], 1, 1) + z_up + z_down)
        return mine, sums

    def edges_of(mine):
        return [jnp.where(col8 == 1, pltpu.roll(m, LANES - 6, 1), m) for m in mine]

    def site_sum(src, q, up, down, z, edges):
        w, j = divmod(z + SITES, SITES)
        fix = pltpu.roll(edges[j], (-(STRIP * w + 2)) % LANES, 1)
        mid = src[q, z + 3]
        right = jnp.where(lane8 == LANES - 1, fix, pltpu.roll(mid, LANES - 1, 1))
        left = jnp.where(lane8 == 0, fix, pltpu.roll(mid, 1, 1))
        return mid, src[up, z + 3] + src[down, z + 3] + right + left + src[q, z + 4] + src[q, z + 2]

    zero = jnp.zeros((PROBES, LANES), jnp.float32)

    def first_level(i, accs):
        e = i - 2
        q, up, down = plane(e), plane(e + 1), plane(e + M - 1)
        mine, sums = strip_sum(s0, q, up, down)
        for j in range(SITES):
            s1[q, j] = se[q, j] * mine[j] - scale * sums[j]
        edges = edges_of(mine)
        one, two = zero, zero
        for z in range(-2, Z + 2):
            mid, total_six = site_sum(v0, q, up, down, z, edges)
            new = en[q, z + 3] * mid - scale * total_six
            v1[q, z + 3] = new
            if 0 <= z < Z:
                one, two = one + mid * new, two + new * new
        own = jnp.where((e >= 0) & (e < X), 1.0, 0.0).astype(jnp.float32)
        return accs[0] + own * one, accs[1] + own * two

    m1, m2 = lax.fori_loop(0, min(M, X + 4), first_level, (zero, zero))

    def second_level(e, acc):
        q, up, down = plane(e), plane(e + 1), plane(e + M - 1)
        mine, sums = strip_sum(s1, q, up, down)
        for j in range(SITES):
            s2[q, j] = 2.0 * (se[q, j] * mine[j] - scale * sums[j]) - s0[q, j]
        edges = edges_of(mine)
        three = zero
        for z in range(-1, Z + 1):
            mid, total_six = site_sum(v1, q, up, down, z, edges)
            new = 2.0 * (en[q, z + 3] * mid - scale * total_six) - v0[q, z + 3]
            v2[q, z + 3] = new
            if 0 <= z < Z:
                three = three + mid * new
        return acc + three

    m3 = lax.fori_loop(0, X, second_level, zero)

    row = zero
    for n, acc in enumerate((m1, m2, m3)):
        summed = jnp.broadcast_to(jnp.sum(acc, axis=1, keepdims=True), (PROBES, LANES))
        row = row + jnp.where(lane8 == PROBES * n + probe, summed, 0.0)
    moms[me] = jnp.sum(row, axis=0, keepdims=True)

    each_other(lambda to: pltpu.make_async_remote_copy(
        src_ref=moms.at[me], dst_ref=moms.at[me], send_sem=msend_sem, recv_sem=mrecv_sem,
        device_id=to, device_id_type=MESH).start())

    def rim_planes(i, _):
        second_level(i * (X + 1) - 1, zero)
        return 0

    lax.fori_loop(0, 2, rim_planes, 0)

    def third_level(x, _):
        q, up, down = plane(x), plane(x + 1), plane(x + M - 1)
        edges = edges_of([s2[q, j] for j in range(SITES)])
        for z in range(Z):
            mid, total_six = site_sum(v2, q, up, down, z, edges)
            new = 2.0 * (en[q, z + 3] * mid - scale * total_six) - v1[q, z + 3]
            at = pl.ds(x * Z + z, PROBES, stride=X * Z)
            prev_ref[at, :] = mid
            cur_ref[at, :] = new
        return 0

    lax.fori_loop(0, X, third_level, 0)

    others = moms.at[pl.ds(0, total - 1)]
    pltpu.make_async_copy(others, others, mrecv_sem).wait()
    pltpu.make_async_copy(others, others, msend_sem).wait()
    sites = total * X * Z * LANES
    sums = jnp.sum(moms[...], axis=0) * (1.0 / sites)
    first = sums
    second = 2.0 * pltpu.roll(sums, LANES - PROBES, 1) - 1.0
    third = 2.0 * pltpu.roll(sums, LANES - 2 * PROBES, 1) - sums
    mom_ref[...] = jnp.concatenate([first, second, third], axis=0)[:, :PROBES]


def write_out(mom_ref, prev_ref, cur_ref, mom_hbm, prev_hbm, cur_hbm, sem):
    copies = [pltpu.make_async_copy(src, dst, sem.at[n]) for n, (src, dst) in enumerate((
        (prev_ref, prev_hbm), (cur_ref, cur_hbm), (mom_ref, mom_hbm)))]
    for copy in copies:
        copy.start()
    for copy in copies:
        copy.wait()


def per_device(names, sizes, probe_bits, disorder_levels):
    X, W, Y = probe_bits.shape
    if Y != LANES or STRIP * (W + 2) > LANES or X < 3:
        raise ValueError("block size")
    Z = SITES * W
    nbx = 2 if sizes["gx"] == 2 else 3
    M = nbx * X
    n_copies = (9 * nbx - 1) + 2 * (3 * nbx - 1)
    total = sizes["gx"] * sizes["gy"] * sizes["gz"]
    rows = (X, W, 1, Y)
    vmem = pl.BlockSpec(memory_space=pltpu.VMEM)
    f32, i32 = jnp.float32, jnp.int32
    tile = (PROBES, LANES)
    hbm = pl.BlockSpec(memory_space=pltpu.HBM)
    out_shape = (
        jax.ShapeDtypeStruct((3, PROBES), f32),
        jax.ShapeDtypeStruct((PROBES * X * Z, Y), f32),
        jax.ShapeDtypeStruct((PROBES * X * Z, Y), f32),
    )
    results = pl.pallas_call(
        functools.partial(kernel, names, sizes),
        out_shape=out_shape,
        in_specs=[hbm] * 4,
        out_specs=(vmem,) * 3,
        scratch_shapes=[
            pltpu.VMEM((X, W, Y), i32),
            pltpu.VMEM((X, W, Y), i32),
            pltpu.VMEM((2, M, W + 2, 1, LANES), i32),
            pltpu.VMEM((nbx, 3, 3, 2 * X, LANES), i32),
            pltpu.VMEM((nbx, 2 * X, LANES), i32),
            pltpu.VMEM((M, Z + 6) + tile, f32),
            pltpu.VMEM((M, Z + 6) + tile, f32),
            pltpu.VMEM((M, Z + 6) + tile, f32),
            pltpu.VMEM((M, Z + 6) + tile, f32),
            pltpu.VMEM((M, SITES) + tile, f32),
            pltpu.VMEM((M, SITES) + tile, f32),
            pltpu.VMEM((M, SITES) + tile, f32),
            pltpu.VMEM((M, SITES) + tile, f32),
            pltpu.VMEM((total, 1, LANES), f32),
            pltpu.SemaphoreType.DMA((4,)),
            pltpu.SemaphoreType.DMA((n_copies,)),
            pltpu.SemaphoreType.DMA((n_copies,)),
            pltpu.SemaphoreType.DMA,
            pltpu.SemaphoreType.DMA,
        ],
        compiler_params=pltpu.CompilerParams(collective_id=0, has_side_effects=True,
                                             vmem_limit_bytes=40 * 1024 * 1024),
    )(probe_bits, disorder_levels, probe_bits.reshape(rows), disorder_levels.reshape(rows))
    moments, previous, current = pl.pallas_call(
        write_out,
        out_shape=out_shape,
        in_specs=[vmem] * 3,
        out_specs=(hbm,) * 3,
        scratch_shapes=[pltpu.SemaphoreType.DMA((3,))],
        compiler_params=pltpu.CompilerParams(vmem_limit_bytes=16 * 1024 * 1024),
    )(*results)
    shape = (PROBES, X, Z, Y)
    return moments, previous.reshape(shape), current.reshape(shape)


def solution(mesh):
    placed = (P("gx", "gz", "gy"), P("gx", "gz", "gy"))
    sizes = {a: mesh.shape[a] for a in mesh.axis_names}
    return jax.shard_map(
        functools.partial(per_device, tuple(mesh.axis_names), sizes),
        mesh=mesh,
        in_specs=placed,
        out_specs=(P(), P(None, "gx", "gz", "gy"), P(None, "gx", "gz", "gy")),
        check_vma=False,
    )
```

```python
import functools

import jax
import jax.numpy as jnp
from jax import lax
from jax.experimental import pallas as pl
from jax.experimental.pallas import tpu as pltpu
from jax.sharding import PartitionSpec as P

PROBES = 8
LEVELS = 256
LANES = 128
SITES = 4
STRIP = 12

disorder_width = 4.0
spectral_scale = 8.4
MESH = pl.DeviceIdType.MESH


def kernel(names, sizes, p_hbm, d_hbm, prow_hbm, drow_hbm, mom_ref, prev_ref, cur_ref,
           p_ref, d_ref, words, packs, strips, v0, v1, v2, en, s0, s1, s2, se, moms,
           load_sem, send_sem, recv_sem, msend_sem, mrecv_sem):
    X, W, _ = p_ref.shape
    Z = SITES * W
    nbx = packs.shape[0]
    M = nbx * X
    gx, gy, gz = sizes["gx"], sizes["gy"], sizes["gz"]
    ix, iy, iz = (lax.axis_index(a) for a in ("gx", "gy", "gz"))
    total = gx * gy * gz
    me = (ix * gy + iy) * gz + iz

    def device(x, y, z):
        at = {"gx": x, "gy": y, "gz": z}
        return tuple(at[a] for a in names)

    loads = [pltpu.make_async_copy(src, dst, load_sem.at[n]) for n, (src, dst) in enumerate((
        (p_hbm, p_ref), (d_hbm, d_ref),
        (prow_hbm, words.at[0, pl.ds(0, X), pl.ds(1, W)]), (drow_hbm, words.at[1, pl.ds(0, X), pl.ds(1, W)])))]
    for load in loads:
        load.start()

    def around(at, size):
        steps = [at]
        for _ in range(size - 1):
            steps.append(jnp.where(steps[-1] + 1 == size, 0, steps[-1] + 1))
        return steps

    around_x, around_y = around(ix, gx), around(iy, gy)

    def each_other(act):
        for x in range(gx):
            for y in range(gy):
                if x or y:
                    act(device(around_x[x], around_y[y], iz))

        def at_depth(z):
            for x in range(gx):
                for y in range(gy):
                    act(device(around_x[x], around_y[y], z))

        if gz <= 4:
            for z in around(iz, gz)[1:]:
                at_depth(z)
        else:
            def step(k, _):
                at_depth(lax.rem(iz + k, gz))
                return 0
            lax.fori_loop(1, gz, step, 0)

    barrier = pltpu.get_barrier_semaphore()
    each_other(lambda to: pl.semaphore_signal(barrier, inc=1, device_id=to, device_id_type=MESH))

    lane = lax.broadcasted_iota(jnp.int32, (2 * X, LANES), 1)
    slot_word = (lane * 10923) >> 17
    column = lane - STRIP * slot_word

    for load in loads:
        load.wait()
    pack = jnp.zeros((2 * X, LANES), jnp.int32)
    for w in range(W):
        rows = jnp.concatenate([p_ref[:, w, :], d_ref[:, w, :]], axis=0)
        base = STRIP * (w + 1)
        first = pltpu.roll(rows, (base - (LANES - 3)) % LANES, 1)
        second = pltpu.roll(rows, (base + 5 - (LANES - 2)) % LANES, 1)
        pack = jnp.where(slot_word == w + 1, jnp.where(column < 5, first, second), pack)
    packs[0, 1, 1] = pack

    pl.semaphore_wait(barrier, total - 1)

    xs = (1, 0) if nbx == 2 else (1, -1, 0)
    near, far = [], []
    slot_of = {0: 0, 1: nbx - 1, -1: 1}
    for ox in xs:
        for oz in (0, 1, -1):
            for oy in (0, 1, -1):
                if ox == 0 and oz == 0 and oy == 0:
                    continue
                to = device(lax.rem(ix + ox + gx, gx), lax.rem(iy + oy + gy, gy), lax.rem(iz + oz + gz, gz))
                s = slot_of[ox]
                moves = []
                if oy == 0:
                    src_w, dst_w = {0: (pl.ds(1, W), pl.ds(1, W)), 1: (pl.ds(W, 1), pl.ds(0, 1)),
                                    -1: (pl.ds(1, 1), pl.ds(W + 1, 1))}[oz]
                    for f in range(2):
                        moves.append((words.at[f, pl.ds(0, X), src_w], words.at[f, pl.ds(s * X, X), dst_w]))
                moves.append((packs.at[0, 1, 1], packs.at[s, 1 - oz, 1 - oy]))
                for src, dst in moves:
                    n = len(near) + len(far)
                    (far if ox else near).append(pltpu.make_async_remote_copy(
                        src_ref=src, dst_ref=dst, send_sem=send_sem.at[n], recv_sem=recv_sem.at[n],
                        device_id=to, device_id_type=MESH))
    for copy in far + near:
        copy.start()
    scale = 1.0 / spectral_scale
    e_mul = disorder_width / LEVELS / spectral_scale
    e_add = disorder_width * (0.5 / LEVELS - 0.5) / spectral_scale
    probe = lax.broadcasted_iota(jnp.int32, (PROBES, LANES), 0)
    lane8 = lax.broadcasted_iota(jnp.int32, (PROBES, LANES), 1)
    col8 = lane8 - STRIP * ((lane8 * 10923) >> 17)
    lifts = [31 - (SITES * probe + j) for j in range(SITES)]

    def sign_of(row, j):
        return jnp.where((jnp.broadcast_to(row, (PROBES, LANES)) << lifts[j]) < 0, 1.0, -1.0).astype(jnp.float32)

    def energy_of(row, j):
        level = (jnp.broadcast_to(row, (PROBES, LANES)) >> (8 * j)) & 255
        return level.astype(jnp.float32) * e_mul + e_add

    def unpack(q, zs):
        for z in zs:
            w, j = divmod(z + SITES, SITES)
            v0[q, z + 3] = sign_of(words[0, q, w], j)
            en[q, z + 3] = energy_of(words[1, q, w], j)

    def unpack_own(x, _):
        unpack(x, range(Z))
        return 0

    lax.fori_loop(0, X, unpack_own, 0)
    for copy in near:
        copy.wait()

    def unpack_strips(s):
        def joined(oz):
            return jnp.where(column < 3, packs[s, oz, 0], jnp.where(column < 7, packs[s, oz, 1], packs[s, oz, 2]))
        strip = jnp.where(slot_word == 0, pltpu.roll(joined(0), (-STRIP * W) % LANES, 1), joined(1))
        strips[s] = jnp.where(slot_word == W + 1, pltpu.roll(joined(2), (STRIP * W) % LANES, 1), strip)
        for x in range(X):
            for j in range(SITES):
                s0[s * X + x, j] = sign_of(strips[s, x:x + 1], j)
                se[s * X + x, j] = energy_of(strips[s, X + x:X + x + 1], j)

    def plane(e):
        return lax.rem(e + M, M)

    def unpack_rim(x, _):
        unpack(x, [*range(-3, 0), *range(Z, Z + 3)])
        return 0

    def unpack_far(i, _):
        unpack(plane(X + i), range(-3, Z + 3))
        return 0

    def unpack_low(i, _):
        unpack(plane(i - 3), range(-3, Z + 3))
        return 0

    unpack_strips(0)
    lax.fori_loop(0, X, unpack_rim, 0)

    def strip_sum(src, q, up, down):
        mine = [src[q, j] for j in range(SITES)]
        sums = []
        for j in range(SITES):
            z_up = mine[j + 1] if j + 1 < SITES else pltpu.roll(mine[0], LANES - STRIP, 1)
            z_down = mine[j - 1] if j > 0 else pltpu.roll(mine[SITES - 1], STRIP, 1)
            sums.append(src[up, j] + src[down, j] + pltpu.roll(mine[j], LANES - 1, 1)
                        + pltpu.roll(mine[j], 1, 1) + z_up + z_down)
        return mine, sums

    def edges_of(mine):
        return [jnp.where(col8 == 1, pltpu.roll(m, LANES - 6, 1), m) for m in mine]

    def site_sum(src, q, up, down, z, edges):
        w, j = divmod(z + SITES, SITES)
        fix = pltpu.roll(edges[j], (-(STRIP * w + 2)) % LANES, 1)
        mid = src[q, z + 3]
        right = jnp.where(lane8 == LANES - 1, fix, pltpu.roll(mid, LANES - 1, 1))
        left = jnp.where(lane8 == 0, fix, pltpu.roll(mid, 1, 1))
        return mid, src[up, z + 3] + src[down, z + 3] + right + left + src[q, z + 4] + src[q, z + 2]

    zero = jnp.zeros((PROBES, LANES), jnp.float32)

    def first_level(e, accs):
        q, up, down = plane(e), plane(e + 1), plane(e + M - 1)
        mine, sums = strip_sum(s0, q, up, down)
        for j in range(SITES):
            s1[q, j] = se[q, j] * mine[j] - scale * sums[j]
        edges = edges_of(mine)
        one, two = zero, zero
        for z in range(-2, Z + 2):
            mid, total_six = site_sum(v0, q, up, down, z, edges)
            new = en[q, z + 3] * mid - scale * total_six
            v1[q, z + 3] = new
            if 0 <= z < Z:
                one, two = one + mid * new, two + new * new
        return accs[0] + one, accs[1] + two

    def first_edge(e):
        def body(i, accs):
            return first_level(i * (X - 1) + e * (1 - 2 * i), accs)
        return body

    accs = lax.fori_loop(1, X - 1, first_level, (zero, zero))
    for copy in far:
        copy.wait()
    for s in range(1, nbx):
        unpack_strips(s)
    if M <= X + 6:
        lax.fori_loop(0, M - X, unpack_far, 0)
    else:
        lax.fori_loop(0, 3, unpack_far, 0)
        lax.fori_loop(0, 3, unpack_low, 0)
    m1, m2 = lax.fori_loop(0, 2, first_edge(0), accs)
    lax.fori_loop(0, 2, first_edge(-1), (zero, zero))

    def second_level(e, acc):
        q, up, down = plane(e), plane(e + 1), plane(e + M - 1)
        mine, sums = strip_sum(s1, q, up, down)
        for j in range(SITES):
            s2[q, j] = 2.0 * (se[q, j] * mine[j] - scale * sums[j]) - s0[q, j]
        edges = edges_of(mine)
        three = zero
        for z in range(-1, Z + 1):
            mid, total_six = site_sum(v1, q, up, down, z, edges)
            new = 2.0 * (en[q, z + 3] * mid - scale * total_six) - v0[q, z + 3]
            v2[q, z + 3] = new
            if 0 <= z < Z:
                three = three + mid * new
        return acc + three

    m3 = lax.fori_loop(0, X, second_level, zero)

    row = zero
    for n, acc in enumerate((m1, m2, m3)):
        summed = jnp.broadcast_to(jnp.sum(acc, axis=1, keepdims=True), (PROBES, LANES))
        row = row + jnp.where(lane8 == PROBES * n + probe, summed, 0.0)
    moms[me] = jnp.sum(row, axis=0, keepdims=True)

    each_other(lambda to: pltpu.make_async_remote_copy(
        src_ref=moms.at[me], dst_ref=moms.at[me], send_sem=msend_sem, recv_sem=mrecv_sem,
        device_id=to, device_id_type=MESH).start())

    lax.fori_loop(0, min(M, X + 4) - (X + 2), first_edge(-2), (zero, zero))

    def rim_planes(i, _):
        second_level(i * (X + 1) - 1, zero)
        return 0

    lax.fori_loop(0, 2, rim_planes, 0)

    def third_level(x, _):
        q, up, down = plane(x), plane(x + 1), plane(x + M - 1)
        edges = edges_of([s2[q, j] for j in range(SITES)])
        for z in range(Z):
            mid, total_six = site_sum(v2, q, up, down, z, edges)
            new = 2.0 * (en[q, z + 3] * mid - scale * total_six) - v1[q, z + 3]
            at = pl.ds(x * Z + z, PROBES, stride=X * Z)
            prev_ref[at, :] = mid
            cur_ref[at, :] = new
        return 0

    lax.fori_loop(0, X, third_level, 0)

    others = moms.at[pl.ds(0, total - 1)]
    pltpu.make_async_copy(others, others, mrecv_sem).wait()
    pltpu.make_async_copy(others, others, msend_sem).wait()
    sites = total * X * Z * LANES
    sums = jnp.sum(moms[...], axis=0) * (1.0 / sites)
    first = sums
    second = 2.0 * pltpu.roll(sums, LANES - PROBES, 1) - 1.0
    third = 2.0 * pltpu.roll(sums, LANES - 2 * PROBES, 1) - sums
    mom_ref[...] = jnp.concatenate([first, second, third], axis=0)[:, :PROBES]


def write_out(mom_ref, prev_ref, cur_ref, mom_hbm, prev_hbm, cur_hbm, sem):
    copies = [pltpu.make_async_copy(src, dst, sem.at[n]) for n, (src, dst) in enumerate((
        (prev_ref, prev_hbm), (cur_ref, cur_hbm), (mom_ref, mom_hbm)))]
    for copy in copies:
        copy.start()
    for copy in copies:
        copy.wait()


def per_device(names, sizes, probe_bits, disorder_levels):
    X, W, Y = probe_bits.shape
    if Y != LANES or STRIP * (W + 2) > LANES or X < 3:
        raise ValueError("block size")
    Z = SITES * W
    nbx = 2 if sizes["gx"] == 2 else 3
    M = nbx * X
    n_copies = (9 * nbx - 1) + 2 * (3 * nbx - 1)
    total = sizes["gx"] * sizes["gy"] * sizes["gz"]
    rows = (X, W, 1, Y)
    vmem = pl.BlockSpec(memory_space=pltpu.VMEM)
    f32, i32 = jnp.float32, jnp.int32
    tile = (PROBES, LANES)
    hbm = pl.BlockSpec(memory_space=pltpu.HBM)
    out_shape = (
        jax.ShapeDtypeStruct((3, PROBES), f32),
        jax.ShapeDtypeStruct((PROBES * X * Z, Y), f32),
        jax.ShapeDtypeStruct((PROBES * X * Z, Y), f32),
    )
    results = pl.pallas_call(
        functools.partial(kernel, names, sizes),
        out_shape=out_shape,
        in_specs=[hbm] * 4,
        out_specs=(vmem,) * 3,
        scratch_shapes=[
            pltpu.VMEM((X, W, Y), i32),
            pltpu.VMEM((X, W, Y), i32),
            pltpu.VMEM((2, M, W + 2, 1, LANES), i32),
            pltpu.VMEM((nbx, 3, 3, 2 * X, LANES), i32),
            pltpu.VMEM((nbx, 2 * X, LANES), i32),
            pltpu.VMEM((M, Z + 6) + tile, f32),
            pltpu.VMEM((M, Z + 6) + tile, f32),
            pltpu.VMEM((M, Z + 6) + tile, f32),
            pltpu.VMEM((M, Z + 6) + tile, f32),
            pltpu.VMEM((M, SITES) + tile, f32),
            pltpu.VMEM((M, SITES) + tile, f32),
            pltpu.VMEM((M, SITES) + tile, f32),
            pltpu.VMEM((M, SITES) + tile, f32),
            pltpu.VMEM((total, 1, LANES), f32),
            pltpu.SemaphoreType.DMA((4,)),
            pltpu.SemaphoreType.DMA((n_copies,)),
            pltpu.SemaphoreType.DMA((n_copies,)),
            pltpu.SemaphoreType.DMA,
            pltpu.SemaphoreType.DMA,
        ],
        compiler_params=pltpu.CompilerParams(collective_id=0, has_side_effects=True,
                                             vmem_limit_bytes=40 * 1024 * 1024),
    )(*[pltpu.with_memory_space_constraint(a, pltpu.HBM) for a in (probe_bits, disorder_levels, probe_bits.reshape(rows), disorder_levels.reshape(rows))])
    moments, previous, current = pl.pallas_call(
        write_out,
        out_shape=out_shape,
        in_specs=[vmem] * 3,
        out_specs=(hbm,) * 3,
        scratch_shapes=[pltpu.SemaphoreType.DMA((3,))],
        compiler_params=pltpu.CompilerParams(vmem_limit_bytes=16 * 1024 * 1024),
    )(*results)
    shape = (PROBES, X, Z, Y)
    return moments, previous.reshape(shape), current.reshape(shape)


def solution(mesh):
    placed = (P("gx", "gz", "gy"), P("gx", "gz", "gy"))
    sizes = {a: mesh.shape[a] for a in mesh.axis_names}
    return jax.shard_map(
        functools.partial(per_device, tuple(mesh.axis_names), sizes),
        mesh=mesh,
        in_specs=placed,
        out_specs=(P(), P(None, "gx", "gz", "gy"), P(None, "gx", "gz", "gy")),
        check_vma=False,
    )
```

```python
import functools

import jax
import jax.numpy as jnp
from jax import lax
from jax.experimental import pallas as pl
from jax.experimental.pallas import tpu as pltpu
from jax.sharding import PartitionSpec as P

PROBES = 8
LEVELS = 256
LANES = 128
SITES = 4
STRIP = 12

disorder_width = 4.0
spectral_scale = 8.4
MESH = pl.DeviceIdType.MESH


def kernel(names, sizes, p_hbm, d_hbm, prow_hbm, drow_hbm, mom_ref, prev_ref, cur_ref,
           p_ref, d_ref, words, packs, strips, v0, v1, v2, en, s0, s1, s2, se, moms,
           load_sem, send_sem, recv_sem, msend_sem, mrecv_sem, ready_sem):
    X, W, _ = p_ref.shape
    Z = SITES * W
    nbx = packs.shape[0]
    M = nbx * X
    gx, gy, gz = sizes["gx"], sizes["gy"], sizes["gz"]
    ix, iy, iz = (lax.axis_index(a) for a in ("gx", "gy", "gz"))
    total = gx * gy * gz
    me = (ix * gy + iy) * gz + iz

    def device(x, y, z):
        at = {"gx": x, "gy": y, "gz": z}
        return tuple(at[a] for a in names)

    loads = [pltpu.make_async_copy(src, dst, load_sem.at[n]) for n, (src, dst) in enumerate((
        (p_hbm, p_ref), (d_hbm, d_ref),
        (prow_hbm, words.at[0, pl.ds(0, X), pl.ds(1, W)]), (drow_hbm, words.at[1, pl.ds(0, X), pl.ds(1, W)])))]
    for load in loads:
        load.start()

    def around(at, size):
        steps = [at]
        for _ in range(size - 1):
            steps.append(jnp.where(steps[-1] + 1 == size, 0, steps[-1] + 1))
        return steps

    around_x, around_y = around(ix, gx), around(iy, gy)

    def each_other(act):
        for x in range(gx):
            for y in range(gy):
                if x or y:
                    act(device(around_x[x], around_y[y], iz))

        def at_depth(z):
            for x in range(gx):
                for y in range(gy):
                    act(device(around_x[x], around_y[y], z))

        if gz <= 4:
            for z in around(iz, gz)[1:]:
                at_depth(z)
        else:
            def step(k, _):
                at_depth(lax.rem(iz + k, gz))
                return 0
            lax.fori_loop(1, gz, step, 0)

    def each_near(act):
        for x in around_x if nbx == 2 else (around_x[0], around_x[1], around_x[-1]):
            for y in (around_y[0], around_y[1], around_y[-1]):
                for z in (iz, lax.rem(iz + 1, gz), lax.rem(iz + gz - 1, gz)):
                    if not (x is ix and y is iy and z is iz):
                        act(device(x, y, z))

    two_steps = max(gx, gy, gz) <= 5
    n_near = 9 * nbx - 1
    barrier = pltpu.get_barrier_semaphore()
    (each_near if two_steps else each_other)(
        lambda to: pl.semaphore_signal(barrier, inc=1, device_id=to, device_id_type=MESH))

    lane = lax.broadcasted_iota(jnp.int32, (2 * X, LANES), 1)
    slot_word = (lane * 10923) >> 17
    column = lane - STRIP * slot_word

    for load in loads:
        load.wait()
    pack = jnp.zeros((2 * X, LANES), jnp.int32)
    for w in range(W):
        rows = jnp.concatenate([p_ref[:, w, :], d_ref[:, w, :]], axis=0)
        base = STRIP * (w + 1)
        first = pltpu.roll(rows, (base - (LANES - 3)) % LANES, 1)
        second = pltpu.roll(rows, (base + 5 - (LANES - 2)) % LANES, 1)
        pack = jnp.where(slot_word == w + 1, jnp.where(column < 5, first, second), pack)
    packs[0, 1, 1] = pack

    pl.semaphore_wait(barrier, n_near if two_steps else total - 1)

    xs = (1, 0) if nbx == 2 else (1, -1, 0)
    near, far = [], []
    slot_of = {0: 0, 1: nbx - 1, -1: 1}
    for ox in xs:
        for oz in (0, 1, -1):
            for oy in (0, 1, -1):
                if ox == 0 and oz == 0 and oy == 0:
                    continue
                to = device(lax.rem(ix + ox + gx, gx), lax.rem(iy + oy + gy, gy), lax.rem(iz + oz + gz, gz))
                s = slot_of[ox]
                moves = []
                if oy == 0:
                    src_w, dst_w = {0: (pl.ds(1, W), pl.ds(1, W)), 1: (pl.ds(W, 1), pl.ds(0, 1)),
                                    -1: (pl.ds(1, 1), pl.ds(W + 1, 1))}[oz]
                    for f in range(2):
                        moves.append((words.at[f, pl.ds(0, X), src_w], words.at[f, pl.ds(s * X, X), dst_w]))
                moves.append((packs.at[0, 1, 1], packs.at[s, 1 - oz, 1 - oy]))
                for src, dst in moves:
                    n = len(near) + len(far)
                    (far if ox else near).append(pltpu.make_async_remote_copy(
                        src_ref=src, dst_ref=dst, send_sem=send_sem.at[n], recv_sem=recv_sem.at[n],
                        device_id=to, device_id_type=MESH))
    for copy in far + near:
        copy.start()
    if two_steps:
        each_near(lambda to: pl.semaphore_signal(ready_sem, inc=1, device_id=to, device_id_type=MESH))
    scale = 1.0 / spectral_scale
    e_mul = disorder_width / LEVELS / spectral_scale
    e_add = disorder_width * (0.5 / LEVELS - 0.5) / spectral_scale
    probe = lax.broadcasted_iota(jnp.int32, (PROBES, LANES), 0)
    lane8 = lax.broadcasted_iota(jnp.int32, (PROBES, LANES), 1)
    col8 = lane8 - STRIP * ((lane8 * 10923) >> 17)
    lifts = [31 - (SITES * probe + j) for j in range(SITES)]

    def sign_of(row, j):
        return jnp.where((jnp.broadcast_to(row, (PROBES, LANES)) << lifts[j]) < 0, 1.0, -1.0).astype(jnp.float32)

    def energy_of(row, j):
        level = (jnp.broadcast_to(row, (PROBES, LANES)) >> (8 * j)) & 255
        return level.astype(jnp.float32) * e_mul + e_add

    def unpack(q, zs):
        for z in zs:
            w, j = divmod(z + SITES, SITES)
            v0[q, z + 3] = sign_of(words[0, q, w], j)
            en[q, z + 3] = energy_of(words[1, q, w], j)

    def unpack_own(x, _):
        unpack(x, range(Z))
        return 0

    lax.fori_loop(0, X, unpack_own, 0)
    for copy in near:
        copy.wait()

    def unpack_strips(s):
        def joined(oz):
            return jnp.where(column < 3, packs[s, oz, 0], jnp.where(column < 7, packs[s, oz, 1], packs[s, oz, 2]))
        strip = jnp.where(slot_word == 0, pltpu.roll(joined(0), (-STRIP * W) % LANES, 1), joined(1))
        strips[s] = jnp.where(slot_word == W + 1, pltpu.roll(joined(2), (STRIP * W) % LANES, 1), strip)
        for x in range(X):
            for j in range(SITES):
                s0[s * X + x, j] = sign_of(strips[s, x:x + 1], j)
                se[s * X + x, j] = energy_of(strips[s, X + x:X + x + 1], j)

    def plane(e):
        return lax.rem(e + M, M)

    def unpack_rim(x, _):
        unpack(x, [*range(-3, 0), *range(Z, Z + 3)])
        return 0

    def unpack_far(i, _):
        unpack(plane(X + i), range(-3, Z + 3))
        return 0

    def unpack_low(i, _):
        unpack(plane(i - 3), range(-3, Z + 3))
        return 0

    unpack_strips(0)
    lax.fori_loop(0, X, unpack_rim, 0)

    def strip_sum(src, q, up, down):
        mine = [src[q, j] for j in range(SITES)]
        sums = []
        for j in range(SITES):
            z_up = mine[j + 1] if j + 1 < SITES else pltpu.roll(mine[0], LANES - STRIP, 1)
            z_down = mine[j - 1] if j > 0 else pltpu.roll(mine[SITES - 1], STRIP, 1)
            sums.append(src[up, j] + src[down, j] + pltpu.roll(mine[j], LANES - 1, 1)
                        + pltpu.roll(mine[j], 1, 1) + z_up + z_down)
        return mine, sums

    def edges_of(mine):
        return [jnp.where(col8 == 1, pltpu.roll(m, LANES - 6, 1), m) for m in mine]

    def site_sum(src, q, up, down, z, edges):
        w, j = divmod(z + SITES, SITES)
        fix = pltpu.roll(edges[j], (-(STRIP * w + 2)) % LANES, 1)
        mid = src[q, z + 3]
        right = jnp.where(lane8 == LANES - 1, fix, pltpu.roll(mid, LANES - 1, 1))
        left = jnp.where(lane8 == 0, fix, pltpu.roll(mid, 1, 1))
        return mid, src[up, z + 3] + src[down, z + 3] + right + left + src[q, z + 4] + src[q, z + 2]

    zero = jnp.zeros((PROBES, LANES), jnp.float32)

    def first_level(e, accs):
        q, up, down = plane(e), plane(e + 1), plane(e + M - 1)
        mine, sums = strip_sum(s0, q, up, down)
        for j in range(SITES):
            s1[q, j] = se[q, j] * mine[j] - scale * sums[j]
        edges = edges_of(mine)
        one, two = zero, zero
        for z in range(-2, Z + 2):
            mid, total_six = site_sum(v0, q, up, down, z, edges)
            new = en[q, z + 3] * mid - scale * total_six
            v1[q, z + 3] = new
            if 0 <= z < Z:
                one, two = one + mid * new, two + new * new
        return accs[0] + one, accs[1] + two

    def first_edge(e):
        def body(i, accs):
            return first_level(i * (X - 1) + e * (1 - 2 * i), accs)
        return body

    accs = lax.fori_loop(1, X - 1, first_level, (zero, zero))
    for copy in far:
        copy.wait()
    for s in range(1, nbx):
        unpack_strips(s)
    if M <= X + 6:
        lax.fori_loop(0, M - X, unpack_far, 0)
    else:
        lax.fori_loop(0, 3, unpack_far, 0)
        lax.fori_loop(0, 3, unpack_low, 0)
    m1, m2 = lax.fori_loop(0, 2, first_edge(0), accs)
    lax.fori_loop(0, 2, first_edge(-1), (zero, zero))

    def second_level(e, acc):
        q, up, down = plane(e), plane(e + 1), plane(e + M - 1)
        mine, sums = strip_sum(s1, q, up, down)
        for j in range(SITES):
            s2[q, j] = 2.0 * (se[q, j] * mine[j] - scale * sums[j]) - s0[q, j]
        edges = edges_of(mine)
        three = zero
        for z in range(-1, Z + 1):
            mid, total_six = site_sum(v1, q, up, down, z, edges)
            new = 2.0 * (en[q, z + 3] * mid - scale * total_six) - v0[q, z + 3]
            v2[q, z + 3] = new
            if 0 <= z < Z:
                three = three + mid * new
        return acc + three

    m3 = lax.fori_loop(0, X, second_level, zero)

    row = zero
    for n, acc in enumerate((m1, m2, m3)):
        summed = jnp.broadcast_to(jnp.sum(acc, axis=1, keepdims=True), (PROBES, LANES))
        row = row + jnp.where(lane8 == PROBES * n + probe, summed, 0.0)
    moms[me] = jnp.sum(row, axis=0, keepdims=True)

    if two_steps:
        pl.semaphore_wait(ready_sem, n_near)
    each_other(lambda to: pltpu.make_async_remote_copy(
        src_ref=moms.at[me], dst_ref=moms.at[me], send_sem=msend_sem, recv_sem=mrecv_sem,
        device_id=to, device_id_type=MESH).start())

    lax.fori_loop(0, min(M, X + 4) - (X + 2), first_edge(-2), (zero, zero))

    def rim_planes(i, _):
        second_level(i * (X + 1) - 1, zero)
        return 0

    lax.fori_loop(0, 2, rim_planes, 0)

    def third_level(x, _):
        q, up, down = plane(x), plane(x + 1), plane(x + M - 1)
        edges = edges_of([s2[q, j] for j in range(SITES)])
        for z in range(Z):
            mid, total_six = site_sum(v2, q, up, down, z, edges)
            new = 2.0 * (en[q, z + 3] * mid - scale * total_six) - v1[q, z + 3]
            at = pl.ds(x * Z + z, PROBES, stride=X * Z)
            prev_ref[at, :] = mid
            cur_ref[at, :] = new
        return 0

    lax.fori_loop(0, X, third_level, 0)

    others = moms.at[pl.ds(0, total - 1)]
    pltpu.make_async_copy(others, others, mrecv_sem).wait()
    pltpu.make_async_copy(others, others, msend_sem).wait()
    sites = total * X * Z * LANES
    sums = jnp.sum(moms[...], axis=0) * (1.0 / sites)
    first = sums
    second = 2.0 * pltpu.roll(sums, LANES - PROBES, 1) - 1.0
    third = 2.0 * pltpu.roll(sums, LANES - 2 * PROBES, 1) - sums
    mom_ref[...] = jnp.concatenate([first, second, third], axis=0)[:, :PROBES]


def write_out(mom_ref, prev_ref, cur_ref, mom_hbm, prev_hbm, cur_hbm, sem):
    copies = [pltpu.make_async_copy(src, dst, sem.at[n]) for n, (src, dst) in enumerate((
        (prev_ref, prev_hbm), (cur_ref, cur_hbm), (mom_ref, mom_hbm)))]
    for copy in copies:
        copy.start()
    for copy in copies:
        copy.wait()


def per_device(names, sizes, probe_bits, disorder_levels):
    X, W, Y = probe_bits.shape
    if Y != LANES or STRIP * (W + 2) > LANES or X < 3:
        raise ValueError("block size")
    Z = SITES * W
    nbx = 2 if sizes["gx"] == 2 else 3
    M = nbx * X
    n_copies = (9 * nbx - 1) + 2 * (3 * nbx - 1)
    total = sizes["gx"] * sizes["gy"] * sizes["gz"]
    rows = (X, W, 1, Y)
    vmem = pl.BlockSpec(memory_space=pltpu.VMEM)
    f32, i32 = jnp.float32, jnp.int32
    tile = (PROBES, LANES)
    hbm = pl.BlockSpec(memory_space=pltpu.HBM)
    out_shape = (
        jax.ShapeDtypeStruct((3, PROBES), f32),
        jax.ShapeDtypeStruct((PROBES * X * Z, Y), f32),
        jax.ShapeDtypeStruct((PROBES * X * Z, Y), f32),
    )
    results = pl.pallas_call(
        functools.partial(kernel, names, sizes),
        out_shape=out_shape,
        in_specs=[hbm] * 4,
        out_specs=(vmem,) * 3,
        scratch_shapes=[
            pltpu.VMEM((X, W, Y), i32),
            pltpu.VMEM((X, W, Y), i32),
            pltpu.VMEM((2, M, W + 2, 1, LANES), i32),
            pltpu.VMEM((nbx, 3, 3, 2 * X, LANES), i32),
            pltpu.VMEM((nbx, 2 * X, LANES), i32),
            pltpu.VMEM((M, Z + 6) + tile, f32),
            pltpu.VMEM((M, Z + 6) + tile, f32),
            pltpu.VMEM((M, Z + 6) + tile, f32),
            pltpu.VMEM((M, Z + 6) + tile, f32),
            pltpu.VMEM((M, SITES) + tile, f32),
            pltpu.VMEM((M, SITES) + tile, f32),
            pltpu.VMEM((M, SITES) + tile, f32),
            pltpu.VMEM((M, SITES) + tile, f32),
            pltpu.VMEM((total, 1, LANES), f32),
            pltpu.SemaphoreType.DMA((4,)),
            pltpu.SemaphoreType.DMA((n_copies,)),
            pltpu.SemaphoreType.DMA((n_copies,)),
            pltpu.SemaphoreType.DMA,
            pltpu.SemaphoreType.DMA,
            pltpu.SemaphoreType.REGULAR,
        ],
        compiler_params=pltpu.CompilerParams(collective_id=0, has_side_effects=True,
                                             vmem_limit_bytes=40 * 1024 * 1024),
    )(*[pltpu.with_memory_space_constraint(a, pltpu.HBM) for a in (probe_bits, disorder_levels, probe_bits.reshape(rows), disorder_levels.reshape(rows))])
    moments, previous, current = pl.pallas_call(
        write_out,
        out_shape=out_shape,
        in_specs=[vmem] * 3,
        out_specs=(hbm,) * 3,
        scratch_shapes=[pltpu.SemaphoreType.DMA((3,))],
        compiler_params=pltpu.CompilerParams(vmem_limit_bytes=16 * 1024 * 1024),
    )(*results)
    shape = (PROBES, X, Z, Y)
    return moments, previous.reshape(shape), current.reshape(shape)


def solution(mesh):
    placed = (P("gx", "gz", "gy"), P("gx", "gz", "gy"))
    sizes = {a: mesh.shape[a] for a in mesh.axis_names}
    return jax.shard_map(
        functools.partial(per_device, tuple(mesh.axis_names), sizes),
        mesh=mesh,
        in_specs=placed,
        out_specs=(P(), P(None, "gx", "gz", "gy"), P(None, "gx", "gz", "gy")),
        check_vma=False,
    )
```
